32 devices in a mesh: dp: 16 (over z, x, core), tensor: 2 (over y).
Axes of the slice: x: 2, y: 2, z: 4, core: 2. Of those that a mesh axis runs over, the one named last changes fastest.
Arguments:
- tokens: bfloat16 [8192, 1536], P(('dp', 'tensor')), may hold values from -6 to 6
- out_grad: bfloat16 [8192, 1536], P(('dp', 'tensor')), may hold values from -6 to 6
- attn_norm: float32 [1536], replicated, may hold values from 0.1 to 1.9
- query_weight: bfloat16 [1536, 1536], P('dp', 'tensor')
- key_weight: bfloat16 [1536, 512], P('dp', 'tensor')
- value_weight: bfloat16 [1536, 512], P('dp', 'tensor'), may hold values from -0.15625 to 0.15625
- output_weight: bfloat16 [1536, 1536], P('dp', 'tensor'), may hold values from -0.625 to 0.625
- moe_norm: float32 [1536], replicated, may hold values from 0.1 to 1.9
- gate_weight: bfloat16 [20, 1536, 512], P(None, 'dp', 'tensor'), may hold values from -0.15625 to 0.15625
- up_weight: bfloat16 [20, 1536, 512], P(None, 'dp', 'tensor'), may hold values from -0.15625 to 0.15625
- down_weight: bfloat16 [20, 1536, 512], P(None, 'dp', 'tensor'), may hold values from -0.5 to 0.5
- expert_ids: int32 [8192, 8], P('dp'), may hold values from 0 to 19, all different within a row; in each aligned block of 512 rows (0 to 511, 512 to 1023, ...) at most 256 rows name the same one
- gate_weights: float32 [8192, 8], P('dp'), may hold values from 0.05 to 0.5
- seq_lengths: int32 [16, 4], P('dp'), may hold values from 0 to 512, as said below
Outputs:
- block_out: bfloat16 [8192, 1536], P(('dp', 'tensor'))
- input_grad: float32 [8192, 1536], P(('dp', 'tensor'))
- grad_attn_norm: float32 [1536], replicated
- grad_query: float32 [1536, 1536], P('dp', 'tensor')
- grad_key: float32 [1536, 512], P('dp', 'tensor')
- grad_value: float32 [1536, 512], P('dp', 'tensor')
- grad_output: float32 [1536, 1536], P('dp', 'tensor')
- grad_moe_norm: float32 [1536], replicated
- grad_gate: float32 [20, 1536, 512], P(None, 'dp', 'tensor')
- grad_up: float32 [20, 1536, 512], P(None, 'dp', 'tensor')
- grad_down: float32 [20, 1536, 512], P(None, 'dp', 'tensor')
The draws below stay inside these ranges and needn't reach their ends.
Inputs may be any that keep to these rules, and one draw needn't show every extreme that they name: `seq_lengths`: each index of dp has 4 entries; a sequence of length n takes the next n rounded up to a multiple of 128 rows of that index, from its first row on, and an entry 0 takes none; the sequences of an index fill between half and all of its 512 rows, and on one index a single sequence fills all of them. `expert_ids`: within the 512 rows of one index of dp each expert is named by at most 256 rows; the 8 entries of a row differ.
All inputs are finite; a program needn't handle non-finite values.
Results may differ from the reference program's by a relative error of at most 0.024.
The reference program's roundings to bfloat16 on the way count: a program that leaves them out, or rounds other values in their place, can miss the bound.
Values may be sent and summed in bfloat16 or wider, within the bound.
A program may use at most 384 MiB of HBM per device.

```python
import math
import jax
import jax.numpy as jnp
import numpy as np
from jax import lax

D = 1536
HEADS = 24
KV_HEADS = 8
HEAD_DIM = 64
EXPERT_FF = 512
TOPK = 8
EXPERTS = 20
BLOCK = 128
SEQ_DEV = 4
TOK_DEV = 512
CAP = 256
TOKENS = 8192
N_DP = 16


def projection_pair(key):
    query_key = jax.random.fold_in(key, 101)
    other_key = jax.random.fold_in(key, 202)
    query_part = jax.random.normal(query_key, (D, HEADS * HEAD_DIM), jnp.float32) * D ** (-0.5)
    key_part = jax.random.normal(other_key, (D, KV_HEADS * HEAD_DIM), jnp.float32) * D ** (-0.5)
    return (query_part, key_part)


def draw_query_weight(key, part):
    return projection_pair(key)[0].astype(jnp.bfloat16)


def draw_key_weight(key, part):
    return projection_pair(key)[1].astype(jnp.bfloat16)


def draw_seq_lengths(key, part):
    block_total = TOK_DEV // BLOCK
    used_key = jax.random.fold_in(key, 1)
    full_key = jax.random.fold_in(key, 2)
    cut_key = jax.random.fold_in(key, 3)
    tail_key = jax.random.fold_in(key, 4)
    used = jax.random.randint(used_key, (N_DP,), block_total // 2, block_total + 1)
    full_index = jax.random.randint(full_key, (), 0, N_DP)
    cuts = jnp.sort(jax.random.randint(cut_key, (N_DP, SEQ_DEV - 1), 0, block_total + 1), axis=1)
    bounds = jnp.concatenate([jnp.zeros((N_DP, 1), jnp.int32), cuts, jnp.full((N_DP, 1), block_total, jnp.int32)], axis=1)
    bounds = jnp.minimum(bounds, used[:, None])
    blocks = bounds[:, 1:] - bounds[:, :-1]
    tails = jax.random.randint(tail_key, (N_DP, SEQ_DEV), 1, BLOCK + 1)
    lengths = jnp.where(blocks > 0, (blocks - 1) * BLOCK + tails, 0)
    single = jnp.concatenate([jnp.full((1,), TOK_DEV, jnp.int32), jnp.zeros((SEQ_DEV - 1,), jnp.int32)])
    lengths = jnp.where(jnp.arange(N_DP, dtype=jnp.int32)[:, None] == full_index, single[None, :], lengths)
    return lengths.astype(jnp.int32)


def level_of(stream_key, dims, shards, least, top_value):
    level = 1.0
    for position, parts in shards:
        steps = jax.random.uniform(jax.random.fold_in(jax.random.fold_in(stream_key, 6), position), (parts,), jnp.float32, least / len(shards), top_value / len(shards))
        level = level * jnp.repeat(jnp.exp(steps), dims[position] // parts).reshape((-1,) + (1,) * (len(dims) - 1 - position))
    return level


def assign_block(key, own, number, rows, number_of, top, most, lean):
    sequence = jax.random.permutation(key, number_of)
    packed, ordinary = load_shares(number_of, rows * top, most, lean, True), load_shares(number_of, rows * top, most, lean, False)
    places = jnp.arange(number_of)

    def named(sizes, rotation):
        used = int((sizes > 0).sum())
        fixed = max(1, used // 4)
        shifted = fixed + (places - fixed + rotation * (used - fixed)) % max(1, number_of - fixed)
        return jnp.zeros((number_of,), jnp.int32).at[sequence[jnp.where(places < fixed, places, shifted)]].set(jnp.asarray(sizes, jnp.int32))

    sizes = jnp.where(number % 4 == 0, named(packed, number // 4), named(ordinary, number - number // 4 - 1))
    mixed = jax.random.permutation(jax.random.fold_in(own, 3), number_of)
    giver, sink = mixed[0:number_of // 2 * 2:2], mixed[1:number_of // 2 * 2:2]
    margin = jnp.minimum(sizes[giver] - 1, most - sizes[sink]) // 2
    margin = jnp.where((giver == sequence[0]) | (sink == sequence[0]) | (sizes[sink] == 0), 0, jnp.maximum(margin, 0))
    shifted = jax.random.randint(jax.random.fold_in(own, 4), (number_of // 2,), 0, 1 << 20) % (margin + 1)
    sizes = sizes.at[giver].add(-shifted).at[sink].add(shifted)
    members = jnp.searchsorted(jnp.cumsum(sizes), jnp.arange(rows * top), side="right").astype(jnp.int32)
    listing = members.reshape(top, rows).T
    listing = listing[jax.random.permutation(jax.random.fold_in(own, 1), rows)]
    rotation = jax.random.randint(jax.random.fold_in(own, 2), (rows, 1), 0, top)
    return jnp.take_along_axis(listing, (jnp.arange(top)[None, :] + rotation) % top, axis=1)


def load_shares(count, total, limit, skew, full):
    portions = [(1 << 20) // math.isqrt(standing ** skew) + 1 for standing in range(1, count + 1)]
    largest = limit if full else min(limit, max(-(-total // count), total * portions[0] // sum(portions)))
    least = 1 if total - largest >= count - 1 else 0
    holding, surplus = [largest] + [least] * (count - 1), total - largest - least * (count - 1)
    while surplus > 0:
        free = [i for i in range(1, count) if holding[i] < largest] or [i for i in range(1, count) if holding[i] < limit]
        pool, left = sum([portions[i] for i in free]), surplus
        for i in free:
            more = min(limit - holding[i], max(1, left * portions[i] // pool), surplus)
            holding[i] = holding[i] + more
            surplus = surplus - more
    return np.array(holding)


def centred(key, extent, spread, reach, shards=(), kind=jnp.bfloat16):
    loudness = level_of(key, extent, shards, -0.22, 0.18) if shards else 1.0
    drawn = jax.random.normal(key, extent, jnp.float32) * spread * loudness
    return jnp.minimum(jnp.maximum(drawn, -reach), reach).astype(kind)


def setup_inputs(seed: int = 0) -> dict:
    streams_of = jax.random.split(jax.random.key(seed), 15)
    tokens = centred(streams_of[0], (TOKENS, D), 1.0, 6.0, ((0, 32),))
    out_grad = centred(streams_of[1], (TOKENS, D), 1.0, 6.0, ((0, 32),))
    attn_norm = jnp.clip(1.0 + 0.18 * jax.random.normal(streams_of[2], (D,), jnp.float32), 0.1, 1.9)
    query_weight = draw_query_weight(jax.random.fold_in(streams_of[14], 71), 0)
    key_weight = draw_key_weight(jax.random.fold_in(streams_of[14], 71), 0)
    value_weight = centred(streams_of[5], (D, KV_HEADS * HEAD_DIM), D ** -0.5, 0.15625, ((0, 16), (1, 2)))
    output_weight = centred(streams_of[6], (D, HEADS * HEAD_DIM), (HEADS * HEAD_DIM // 16) ** -0.5, 0.625, ((0, 16), (1, 2)))
    moe_norm = jnp.clip(1.0 + 0.18 * jax.random.normal(streams_of[7], (D,), jnp.float32), 0.1, 1.9)
    gate_weight = centred(streams_of[8], (EXPERTS, D, EXPERT_FF), D ** -0.5, 0.15625, ((1, 16), (2, 2)))
    up_weight = centred(streams_of[9], (EXPERTS, D, EXPERT_FF), D ** -0.5, 0.15625, ((1, 16), (2, 2)))
    down_weight = centred(streams_of[10], (EXPERTS, D, EXPERT_FF), (EXPERT_FF // 4) ** -0.5, 0.5, ((1, 16), (2, 2)))
    expert_ids_keys = jax.random.split(jax.random.fold_in(streams_of[11], 1), TOKENS // TOK_DEV)
    expert_ids_turns = jax.random.permutation(jax.random.fold_in(streams_of[11], 3), TOKENS // TOK_DEV)
    expert_ids = jax.vmap(lambda own, number: assign_block(jax.random.fold_in(streams_of[11], 2), own, number, TOK_DEV, EXPERTS, TOPK, CAP, 1))(expert_ids_keys, expert_ids_turns).reshape((TOKENS, TOPK))
    gate_weights = jnp.clip(0.05 + 0.45 * jax.random.uniform(streams_of[12], (TOKENS, TOPK), jnp.float32) ** level_of(streams_of[12], (TOKENS, TOPK), ((0, 16),), -0.2, 0.2), 0.05, 0.5)
    seq_lengths = draw_seq_lengths(jax.random.fold_in(streams_of[14], 71), 0)
    return {"tokens": tokens, "out_grad": out_grad, "attn_norm": attn_norm, "query_weight": query_weight, "key_weight": key_weight, "value_weight": value_weight, "output_weight": output_weight, "moe_norm": moe_norm, "gate_weight": gate_weight, "up_weight": up_weight, "down_weight": down_weight, "expert_ids": expert_ids, "gate_weights": gate_weights, "seq_lengths": seq_lengths}


EPSILON = 1e-06
ROPE_BASE = 10000.0
MASKED = -1e+30

def batched(pattern, first_op, second_op):
    return jnp.einsum(pattern, first_op.astype(jnp.float32), second_op.astype(jnp.float32))

def times_t(first_op, weight):
    return jnp.dot(first_op, weight.T, preferred_element_type=jnp.float32)

def plain_dot(first_op, weight):
    return jnp.dot(first_op, weight, preferred_element_type=jnp.float32)

def inner_rows(first_op, second_op):
    return jnp.dot(first_op.T, second_op, preferred_element_type=jnp.float32)

def rms_rows(widened):
    inv_rms = lax.rsqrt(lax.optimization_barrier(jnp.mean(widened * widened, axis=-1, keepdims=True)) + EPSILON)
    return (widened * inv_rms, inv_rms)

def norm_back(grad_in, unit_rows, inv_rms, gain):
    scaled = grad_in * gain
    back = inv_rms * (scaled - unit_rows * lax.optimization_barrier(jnp.mean(scaled * unit_rows, axis=-1, keepdims=True)))
    return (back, lax.optimization_barrier(jnp.sum(grad_in * unit_rows, axis=0)))

def row_layout(lengths, row_count):
    padded = (lengths + BLOCK - 1) // BLOCK * BLOCK
    seq_ends = jnp.cumsum(padded).astype(jnp.int32)
    starts = seq_ends - padded
    row_ids = jnp.arange(row_count, dtype=jnp.int32)
    doc_ids = lax.optimization_barrier(jnp.sum((row_ids[:, None] >= seq_ends[None, :]).astype(jnp.int32), axis=1)).astype(jnp.int32)
    chosen = doc_ids[:, None] == jnp.arange(lengths.shape[0], dtype=jnp.int32)[None, :]
    first_row = lax.optimization_barrier(jnp.sum(jnp.where(chosen, starts[None, :], 0), axis=1)).astype(jnp.int32)
    length_row = lax.optimization_barrier(jnp.sum(jnp.where(chosen, lengths[None, :], 0), axis=1)).astype(jnp.int32)
    positions = row_ids - first_row
    return (doc_ids, positions, positions < length_row)

def rope_tables(positions, width):
    frequency = jnp.exp(jnp.arange(width // 2, dtype=jnp.int32).astype(jnp.float32) * (-2.0 * math.log(ROPE_BASE) / width))
    angles = positions.astype(jnp.float32)[:, None] * frequency[None, :]
    cosine = jnp.cos(angles)
    sine_table = jnp.sin(angles)
    return (jnp.concatenate([cosine, cosine], axis=1), jnp.concatenate([sine_table, sine_table], axis=1))

def rotate(values, cosine, sine_table):
    half_width = values.shape[-1] // 2
    turned = jnp.concatenate([-values[..., half_width:], values[..., :half_width]], axis=-1)
    return values * cosine[:, None, :] + turned * sine_table[:, None, :]

def rotate_back(grads, cosine, sine_table):
    half_width = grads.shape[-1] // 2
    turned = jnp.concatenate([grads[..., half_width:], -grads[..., :half_width]], axis=-1)
    return grads * cosine[:, None, :] + turned * sine_table[:, None, :]

def block_span(row_count):
    return min(512, row_count)

def allowed_block(first_row, block_rows, doc_ids, live_rows):
    row_count = doc_ids.shape[0]
    query_rows = first_row + jnp.arange(block_rows, dtype=jnp.int32)
    key_rows = jnp.arange(row_count, dtype=jnp.int32)
    query_doc = lax.dynamic_slice_in_dim(doc_ids, first_row, block_rows)
    query_live = lax.dynamic_slice_in_dim(live_rows, first_row, block_rows)
    same_doc = (key_rows[None, :] <= query_rows[:, None]) & (doc_ids[None, :] == query_doc[:, None])
    same_doc = same_doc & live_rows[None, :] & query_live[:, None]
    return same_doc | (key_rows[None, :] == query_rows[:, None])

def attend(queries, keys_rot, values, doc_ids, live_rows):
    row_count, head_count, head_width = queries.shape
    group_size = head_count // keys_rot.shape[1]
    keys_wide = jnp.repeat(keys_rot, group_size, axis=1)
    values_wide = jnp.repeat(values, group_size, axis=1)
    block_rows = block_span(row_count)
    block_count = row_count // block_rows
    score_scale = head_width ** (-0.5)

    def one_block(block_index):
        first_row = block_index * block_rows
        query_blk = lax.dynamic_slice_in_dim(queries, first_row, block_rows, 0)
        scores = batched('qhd,khd->hqk', query_blk, keys_wide) * score_scale
        scores = jnp.where(allowed_block(first_row, block_rows, doc_ids, live_rows)[None], scores, MASKED)
        highest = lax.optimization_barrier(jnp.max(scores, axis=-1, keepdims=True))
        weights_exp = jnp.exp(scores - highest)
        totals = lax.optimization_barrier(jnp.sum(weights_exp, axis=-1, keepdims=True))
        probability = (weights_exp / totals).astype(jnp.bfloat16)
        log_total = (highest + jnp.log(totals))[:, :, 0]
        return (batched('hqk,khd->qhd', probability, values_wide).astype(jnp.bfloat16), log_total)
    attn_blocks, log_totals = lax.map(one_block, jnp.arange(block_count, dtype=jnp.int32))
    return (attn_blocks.reshape(row_count, head_count, head_width), log_totals)

def attend_back(queries, keys_rot, values, attn_rows, log_totals, attn_grad, doc_ids, live_rows):
    row_count, head_count, head_width = queries.shape
    kv_count = keys_rot.shape[1]
    group_size = head_count // kv_count
    keys_wide = jnp.repeat(keys_rot, group_size, axis=1)
    values_wide = jnp.repeat(values, group_size, axis=1)
    block_rows = block_span(row_count)
    block_count = row_count // block_rows
    score_scale = head_width ** (-0.5)

    def one_block(running, block_index):
        key_acc, value_acc = running
        first_row = block_index * block_rows
        query_blk = lax.dynamic_slice_in_dim(queries, first_row, block_rows, 0)
        attn_blk = lax.dynamic_slice_in_dim(attn_rows, first_row, block_rows, 0)
        grad_blk = lax.dynamic_slice_in_dim(attn_grad, first_row, block_rows, 0)
        scores = batched('qhd,khd->hqk', query_blk, keys_wide) * score_scale
        scores = jnp.where(allowed_block(first_row, block_rows, doc_ids, live_rows)[None], scores, MASKED)
        probability = jnp.exp(scores - log_totals[block_index][:, :, None])
        value_acc = value_acc + batched('hqk,qhd->khd', probability.astype(jnp.bfloat16), grad_blk)
        through = batched('qhd,khd->hqk', grad_blk, values_wide)
        diagonal = lax.optimization_barrier(jnp.sum(grad_blk.astype(jnp.float32) * attn_blk.astype(jnp.float32), axis=-1)).T
        score_grad = (probability * (through - diagonal[:, :, None])).astype(jnp.bfloat16)
        query_grad = batched('hqk,khd->qhd', score_grad, keys_wide) * score_scale
        key_acc = key_acc + batched('hqk,qhd->khd', score_grad, query_blk) * score_scale
        return ((key_acc, value_acc), query_grad)
    zero_heads = jnp.zeros((row_count, head_count, head_width), jnp.float32)
    (key_acc, value_acc), query_grads = lax.scan(one_block, (zero_heads, zero_heads), jnp.arange(block_count, dtype=jnp.int32))
    query_grad = query_grads.reshape(row_count, head_count, head_width)
    key_grad = key_acc.reshape(row_count, kv_count, group_size, head_width).sum(axis=2)
    value_grad = value_acc.reshape(row_count, kv_count, group_size, head_width).sum(axis=2)
    return (query_grad, key_grad, value_grad)

def slot_map(expert_ids, live_rows, gate_weights, expert_count, capacity):
    row_count, top_count = expert_ids.shape
    flat_ids = expert_ids.reshape(-1)
    valid_pair = jnp.repeat(live_rows, top_count)
    onehot = ((flat_ids[:, None] == jnp.arange(expert_count, dtype=jnp.int32)[None, :]) & valid_pair[:, None]).astype(jnp.int32)
    slot_rank = lax.optimization_barrier(jnp.sum(jnp.cumsum(onehot, axis=0).astype(jnp.int32) * onehot, axis=1)).astype(jnp.int32) - 1
    target = jnp.where(valid_pair, flat_ids * capacity + slot_rank, expert_count * capacity)
    token_rows = jnp.repeat(jnp.arange(row_count, dtype=jnp.int32), top_count)
    sources = jnp.full((expert_count * capacity + 1,), row_count, jnp.int32).at[target].set(token_rows)
    slot_gate = jnp.zeros((expert_count * capacity + 1,), jnp.float32).at[target].set(gate_weights.reshape(-1))
    return (sources[:-1].reshape(expert_count, capacity), slot_gate[:-1].reshape(expert_count, capacity))

def silu_parts(gate_pre):
    sigma = jax.nn.sigmoid(gate_pre)
    return (gate_pre * sigma, sigma * (1.0 + gate_pre * (1.0 - sigma)))

def expert_forward(expert_in, sources, slot_gate, gate_full, up_full, down_full):
    row_count, width = expert_in.shape
    padded_rows = jnp.concatenate([expert_in, jnp.zeros((1, width), expert_in.dtype)], axis=0)

    def one_expert(accum, item):
        source_e, gate_e, gate_w, up_w, down_w = item
        rows_e = padded_rows[source_e]
        gate_pre = plain_dot(rows_e, gate_w)
        up_pre = plain_dot(rows_e, up_w)
        activ = (silu_parts(gate_pre)[0] * up_pre).astype(jnp.bfloat16)
        result = times_t(activ, down_w)
        accum = accum.at[source_e].add(result * gate_e[:, None])
        return (accum, (gate_pre, up_pre))
    accum, kept = lax.scan(one_expert, jnp.zeros((row_count + 1, width), jnp.float32), (sources, slot_gate, gate_full, up_full, down_full))
    return (accum[:row_count], kept)

def expert_backward(expert_in, grad_rows, sources, slot_gate, gate_full, up_full, down_full, kept):
    row_count, width = expert_in.shape
    padded_rows = jnp.concatenate([expert_in, jnp.zeros((1, width), expert_in.dtype)], axis=0)
    padded_grads = jnp.concatenate([grad_rows, jnp.zeros((1, width), grad_rows.dtype)], axis=0)

    def one_expert(accum, item):
        source_e, gate_e, gate_w, up_w, down_w, gate_pre, up_pre = item
        slot_grad = (padded_grads[source_e].astype(jnp.float32) * gate_e[:, None]).astype(jnp.bfloat16)
        act_grad = plain_dot(slot_grad, down_w)
        silu_val, slope = silu_parts(gate_pre)
        activ = (silu_val * up_pre).astype(jnp.bfloat16)
        gate_grad = (act_grad * up_pre * slope).astype(jnp.bfloat16)
        up_grad = (act_grad * silu_val).astype(jnp.bfloat16)
        rows_e = padded_rows[source_e]
        grad_d = inner_rows(slot_grad, activ)
        grad_g = inner_rows(rows_e, gate_grad)
        grad_u = inner_rows(rows_e, up_grad)
        back = times_t(gate_grad, gate_w) + times_t(up_grad, up_w)
        accum = accum.at[source_e].add(back)
        return (accum, (grad_g, grad_u, grad_d))
    accum, grads = lax.scan(one_expert, jnp.zeros((row_count + 1, width), jnp.float32), (sources, slot_gate, gate_full, up_full, down_full, kept[0], kept[1]))
    return (accum[:row_count], grads)

def layer_pass(tokens, out_grad, attn_norm, query_weight, key_weight, value_weight, output_weight, moe_norm, gate_weight, up_weight, down_weight, expert_ids, gate_weights, lengths):
    row_count = tokens.shape[0]
    doc_ids, positions, live_rows = row_layout(lengths, row_count)
    cosine, sine_table = rope_tables(positions, HEAD_DIM)
    widened = tokens.astype(jnp.float32)
    unit_attn, inv_attn = rms_rows(widened)
    normed = (unit_attn * attn_norm).astype(jnp.bfloat16)
    head_count = query_weight.shape[1] // HEAD_DIM
    kv_count = key_weight.shape[1] // HEAD_DIM
    queries = rotate(plain_dot(normed, query_weight).reshape(row_count, head_count, HEAD_DIM), cosine, sine_table).astype(jnp.bfloat16)
    keys_rot = rotate(plain_dot(normed, key_weight).reshape(row_count, kv_count, HEAD_DIM), cosine, sine_table).astype(jnp.bfloat16)
    values = plain_dot(normed, value_weight).astype(jnp.bfloat16).reshape(row_count, kv_count, HEAD_DIM)
    attn_rows, log_totals = attend(queries, keys_rot, values, doc_ids, live_rows)
    attn_flat = attn_rows.reshape(row_count, head_count * HEAD_DIM)
    after_attn = widened + times_t(attn_flat, output_weight)
    unit_moe, inv_moe = rms_rows(after_attn)
    expert_in = (unit_moe * moe_norm).astype(jnp.bfloat16)
    sources, slot_gate = slot_map(expert_ids, live_rows, gate_weights, gate_weight.shape[0], CAP)
    mixed, kept = expert_forward(expert_in, sources, slot_gate, gate_weight, up_weight, down_weight)
    block_out = (after_attn + mixed).astype(jnp.bfloat16)
    moe_grad, expert_grads = expert_backward(expert_in, out_grad, sources, slot_gate, gate_weight, up_weight, down_weight, kept)
    back_moe, grad_moe_norm = norm_back(moe_grad, unit_moe, inv_moe, moe_norm)
    resid_grad = out_grad.astype(jnp.float32) + back_moe
    resid_half = resid_grad.astype(jnp.bfloat16)
    grad_output = inner_rows(resid_half, attn_flat)
    attn_grad = plain_dot(resid_half, output_weight).astype(jnp.bfloat16).reshape(row_count, head_count, HEAD_DIM)
    query_grad, key_grad, value_grad = attend_back(queries, keys_rot, values, attn_rows, log_totals, attn_grad, doc_ids, live_rows)
    query_pre = rotate_back(query_grad, cosine, sine_table).astype(jnp.bfloat16).reshape(row_count, -1)
    key_pre = rotate_back(key_grad, cosine, sine_table).astype(jnp.bfloat16).reshape(row_count, -1)
    value_pre = value_grad.astype(jnp.bfloat16).reshape(row_count, -1)
    grad_query = inner_rows(normed, query_pre)
    grad_key = inner_rows(normed, key_pre)
    grad_value = inner_rows(normed, value_pre)
    attn_in_grad = times_t(query_pre, query_weight) + times_t(key_pre, key_weight) + times_t(value_pre, value_weight)
    back_attn, grad_attn_norm = norm_back(attn_in_grad, unit_attn, inv_attn, attn_norm)
    input_grad = resid_grad + back_attn
    grads = (grad_attn_norm, grad_query, grad_key, grad_value, grad_output, grad_moe_norm, expert_grads[0], expert_grads[1], expert_grads[2])
    return (block_out, input_grad, grads)

def reference(tokens, out_grad, attn_norm, query_weight, key_weight, value_weight, output_weight, moe_norm, gate_weight, up_weight, down_weight, expert_ids, gate_weights, seq_lengths):
    stacked = (tokens.reshape(N_DP, TOK_DEV, D), out_grad.reshape(N_DP, TOK_DEV, D), expert_ids.reshape(N_DP, TOK_DEV, TOPK), gate_weights.reshape(N_DP, TOK_DEV, TOPK), seq_lengths)
    totals = tuple((jnp.zeros(param.shape, jnp.float32) for param in (attn_norm, query_weight, key_weight, value_weight, output_weight, moe_norm, gate_weight, up_weight, down_weight)))

    def one_index(running, item):
        tok_rows, grad_rows, id_rows, gate_rows, lengths = item
        block_out, input_grad, grads = layer_pass(tok_rows, grad_rows, attn_norm, query_weight, key_weight, value_weight, output_weight, moe_norm, gate_weight, up_weight, down_weight, id_rows, gate_rows, lengths)
        return (tuple((part + term for part, term in zip(running, grads))), (block_out, input_grad))
    sums, (outs_all, grads_all) = lax.scan(one_index, totals, stacked)
    return (outs_all.reshape(TOKENS, D), grads_all.reshape(TOKENS, D), sums[0], sums[1], sums[2], sums[3], sums[4], sums[5], sums[6], sums[7], sums[8])
```

```python
import functools
import math

import jax
import jax.numpy as jnp
from jax import lax
from jax.experimental import pallas as pl
from jax.experimental.pallas import tpu as pltpu
from jax.sharding import PartitionSpec as P

HEAD_DIM = 64
BLOCK = 128
GATHERS = 2
PASSES = 4


EPSILON = 1e-06
ROPE_BASE = 10000.0
MASKED = -1e30


def batched(pattern, first_op, second_op):
    return jnp.einsum(pattern, first_op, second_op, preferred_element_type=jnp.float32)


def times_t(first_op, weight):
    return lax.dot_general(
        first_op, weight, (((1,), (1,)), ((), ())), preferred_element_type=jnp.float32
    )


def plain_dot(first_op, weight):
    return jnp.dot(first_op, weight, preferred_element_type=jnp.float32)


def inner_rows(first_op, second_op):
    return lax.dot_general(
        first_op, second_op, (((0,), (0,)), ((), ())), preferred_element_type=jnp.float32
    )


def rms_rows(widened):
    inv_rms = lax.rsqrt(jnp.mean(widened * widened, axis=-1, keepdims=True) + EPSILON)
    return (widened * inv_rms, inv_rms)


def norm_back(grad_in, unit_rows, inv_rms, gain):
    scaled = grad_in * gain
    back = inv_rms * (scaled - unit_rows * jnp.mean(scaled * unit_rows, axis=-1, keepdims=True))
    return (back, jnp.sum(grad_in * unit_rows, axis=0))


def row_layout(lengths, row_count):
    padded = (lengths + BLOCK - 1) // BLOCK * BLOCK
    seq_ends = jnp.cumsum(padded)
    starts = seq_ends - padded
    row_ids = jnp.arange(row_count, dtype=jnp.int32)
    doc_ids = jnp.sum((row_ids[:, None] >= seq_ends[None, :]).astype(jnp.int32), axis=1)
    chosen = doc_ids[:, None] == jnp.arange(lengths.shape[0], dtype=jnp.int32)[None, :]
    first_row = jnp.sum(jnp.where(chosen, starts[None, :], 0), axis=1)
    length_row = jnp.sum(jnp.where(chosen, lengths[None, :], 0), axis=1)
    positions = row_ids - first_row
    return (doc_ids, positions, positions < length_row)


def rope_tables(positions, width):
    frequency = jnp.exp(
        jnp.arange(width // 2, dtype=jnp.int32).astype(jnp.float32)
        * (-2.0 * math.log(ROPE_BASE) / width)
    )
    angles = positions.astype(jnp.float32)[:, None] * frequency[None, :]
    cosine = jnp.cos(angles)
    sine_table = jnp.sin(angles)
    return (
        jnp.concatenate([cosine, cosine], axis=1),
        jnp.concatenate([sine_table, sine_table], axis=1),
    )


def rotate(values, cosine, sine_table):
    half_width = values.shape[-1] // 2
    turned = jnp.concatenate([-values[..., half_width:], values[..., :half_width]], axis=-1)
    return values * cosine[:, None, :] + turned * sine_table[:, None, :]


def rotate_back(grads, cosine, sine_table):
    half_width = grads.shape[-1] // 2
    turned = jnp.concatenate([grads[..., half_width:], -grads[..., :half_width]], axis=-1)
    return grads * cosine[:, None, :] + turned * sine_table[:, None, :]


def block_span(row_count):
    return min(512, row_count)


def allowed_block(first_row, block_rows, doc_ids, live_rows):
    row_count = doc_ids.shape[0]
    query_rows = first_row + jnp.arange(block_rows, dtype=jnp.int32)
    key_rows = jnp.arange(row_count, dtype=jnp.int32)
    same_doc = (key_rows[None, :] <= query_rows[:, None]) & (doc_ids[None, :] == doc_ids[:, None])
    same_doc = same_doc & live_rows[None, :] & live_rows[:, None]
    return same_doc | (key_rows[None, :] == query_rows[:, None])


def attend(queries, keys_rot, values, doc_ids, live_rows):
    row_count, head_count, head_width = queries.shape
    group_size = head_count // keys_rot.shape[1]
    keys_wide = jnp.repeat(keys_rot, group_size, axis=1)
    values_wide = jnp.repeat(values, group_size, axis=1)
    block_rows = block_span(row_count)
    block_count = row_count // block_rows
    score_scale = head_width ** (-0.5)

    def one_block(block_index):
        first_row = block_index * block_rows
        scores = batched("qhd,khd->hqk", queries, keys_wide) * score_scale
        scores = jnp.where(
            allowed_block(first_row, block_rows, doc_ids, live_rows)[None], scores, MASKED
        )
        highest = jnp.max(scores, axis=-1, keepdims=True)
        weights_exp = jnp.exp(scores - highest)
        totals = jnp.sum(weights_exp, axis=-1, keepdims=True)
        probability = (weights_exp / totals).astype(jnp.bfloat16)
        log_total = (highest + jnp.log(totals))[:, :, 0]
        return (batched("hqk,khd->qhd", probability, values_wide).astype(jnp.bfloat16), log_total)

    attn_blocks, log_totals = lax.map(one_block, jnp.arange(block_count, dtype=jnp.int32))
    return (attn_blocks.reshape(row_count, head_count, head_width), log_totals)


def attend_back(queries, keys_rot, values, attn_rows, log_totals, attn_grad, doc_ids, live_rows):
    row_count, head_count, head_width = queries.shape
    kv_count = keys_rot.shape[1]
    group_size = head_count // kv_count
    keys_wide = jnp.repeat(keys_rot, group_size, axis=1)
    values_wide = jnp.repeat(values, group_size, axis=1)
    block_rows = block_span(row_count)
    block_count = row_count // block_rows
    score_scale = head_width ** (-0.5)

    def one_block(running, block_index):
        key_acc, value_acc = running
        first_row = block_index * block_rows
        scores = batched("qhd,khd->hqk", queries, keys_wide) * score_scale
        scores = jnp.where(
            allowed_block(first_row, block_rows, doc_ids, live_rows)[None], scores, MASKED
        )
        probability = jnp.exp(scores - log_totals[block_index][:, :, None])
        value_acc = value_acc + batched("hqk,qhd->khd", probability.astype(jnp.bfloat16), attn_grad)
        through = batched("qhd,khd->hqk", attn_grad, values_wide)
        diagonal = jnp.sum(attn_grad.astype(jnp.float32) * attn_rows.astype(jnp.float32), axis=-1).T
        score_grad = (probability * (through - diagonal[:, :, None])).astype(jnp.bfloat16)
        query_grad = batched("hqk,khd->qhd", score_grad, keys_wide) * score_scale
        key_acc = key_acc + batched("hqk,qhd->khd", score_grad, queries) * score_scale
        return ((key_acc, value_acc), query_grad)

    zero_heads = jnp.zeros((row_count, head_count, head_width), jnp.float32)
    (key_acc, value_acc), query_grads = lax.scan(
        one_block, (zero_heads, zero_heads), jnp.arange(block_count, dtype=jnp.int32)
    )
    query_grad = query_grads.reshape(row_count, head_count, head_width)
    key_grad = key_acc.reshape(row_count, kv_count, group_size, head_width).sum(axis=2)
    value_grad = value_acc.reshape(row_count, kv_count, group_size, head_width).sum(axis=2)
    return (query_grad, key_grad, value_grad)


def silu_parts(gate_pre):
    sigma = jax.nn.sigmoid(gate_pre)
    return (gate_pre * sigma, sigma * (1.0 + gate_pre * (1.0 - sigma)))


def expert_gates(expert_ids, gate_weights, live_rows, expert_count):
    named = expert_ids[:, :, None] == jnp.arange(expert_count, dtype=jnp.int32)[None, None, :]
    named = named & live_rows[:, None, None]
    return jnp.sum(jnp.where(named, gate_weights[:, :, None], 0.0), axis=1)


def expert_kernel(
    first_expert,
    row_tile,
    feat_tile,
    rows_ref,
    rows_t_ref,
    grads_ref,
    grads_t_ref,
    gates_ref,
    gates_t_ref,
    weights_ref,
    mix_in_ref,
    back_in_ref,
    mix_ref,
    back_ref,
    out_ref,
    act_ref,
    pair_ref,
):
    step = pl.program_id(0)
    expert = first_expert + step
    row_count, width = rows_ref.shape
    depth, hidden = weights_ref.shape[3:]

    @pl.when(step == 0)
    def _():
        mix_ref[...] = mix_in_ref[...]
        back_ref[...] = back_in_ref[...]

    gate_w = weights_ref[:, 0, 0].reshape(width, hidden)
    up_w = weights_ref[:, 1, 0].reshape(width, hidden)
    down_w = weights_ref[:, 2, 0].reshape(width, hidden)
    lanes = lax.broadcasted_iota(jnp.int32, (row_tile, gates_ref.shape[1]), 1)
    for start in range(0, row_count, row_tile):
        rows = slice(start, start + row_tile)
        gate_col = jnp.sum(
            jnp.where(lanes == expert, gates_ref[rows, :], 0.0), axis=1, keepdims=True
        )
        gate_pre = plain_dot(rows_ref[rows, :], gate_w)
        up_pre = plain_dot(rows_ref[rows, :], up_w)
        silu_val, slope = silu_parts(gate_pre)
        activ = (silu_val * up_pre).astype(jnp.bfloat16)
        act_ref[rows, :] = activ
        slot_grad = (grads_ref[rows, :].astype(jnp.float32) * gate_col).astype(jnp.bfloat16)
        act_grad = plain_dot(slot_grad, down_w)
        gate_grad = (act_grad * up_pre * slope).astype(jnp.bfloat16)
        up_grad = (act_grad * silu_val).astype(jnp.bfloat16)
        pair_ref[rows, :hidden] = gate_grad
        pair_ref[rows, hidden:] = up_grad
        mix_ref[rows, :] += times_t(activ, down_w) * gate_col
        back_ref[rows, :] += times_t(gate_grad, gate_w) + times_t(up_grad, up_w)
    gate_row = gates_t_ref[pl.ds(expert, 1), :]
    per_tile = feat_tile // depth
    for tile in range(width // feat_tile):
        feats = slice(tile * feat_tile, (tile + 1) * feat_tile)
        parts = slice(tile * per_tile, (tile + 1) * per_tile)
        pair = plain_dot(rows_t_ref[feats, :], pair_ref[...]).astype(jnp.bfloat16)
        out_ref[parts, 0, 0] = pair[:, :hidden].reshape(per_tile, depth, hidden)
        out_ref[parts, 1, 0] = pair[:, hidden:].reshape(per_tile, depth, hidden)
        slot_grad_t = (grads_t_ref[feats, :].astype(jnp.float32) * gate_row).astype(jnp.bfloat16)
        down = plain_dot(slot_grad_t, act_ref[...]).astype(jnp.bfloat16)
        out_ref[parts, 2, 0] = down.reshape(per_tile, depth, hidden)


def expert_pass(first_expert, count, offset, rows, rows_t, grads, grads_t, gates, gates_t, weights, mix, back):
    shards, kinds, held, depth, hidden = weights.shape
    row_count, width = rows.shape
    packed = depth % 16 != 0
    if packed:
        weights = weights.transpose(1, 2, 0, 3, 4).reshape(1, kinds, held, width, hidden)
    groups, inner = weights.shape[0], weights.shape[3]
    feat_tile = inner
    while feat_tile < 384 and (width // feat_tile) % 2 == 0:
        feat_tile *= 2

    def whole(array):
        return pl.BlockSpec(array.shape, lambda i: (0,) * array.ndim, pipeline_mode=pl.Buffered(1))

    shape = (groups, kinds, 1, inner, hidden)
    block = pl.BlockSpec(shape, lambda i: (0, 0, i + offset, 0, 0))
    out_block = pl.BlockSpec(shape, lambda i: (0, 0, i, 0, 0))
    fixed = (rows, rows_t, grads, grads_t, gates, gates_t)
    mix, back, out = pl.pallas_call(
        functools.partial(expert_kernel, first_expert, min(256, row_count), feat_tile),
        grid=(count,),
        in_specs=[whole(a) for a in fixed] + [block, whole(mix), whole(back)],
        out_specs=[whole(mix), whole(back), out_block],
        out_shape=[
            jax.ShapeDtypeStruct(mix.shape, mix.dtype),
            jax.ShapeDtypeStruct(back.shape, back.dtype),
            jax.ShapeDtypeStruct((groups, kinds, count, inner, hidden), jnp.bfloat16),
        ],
        scratch_shapes=[
            pltpu.VMEM((row_count, hidden), jnp.bfloat16),
            pltpu.VMEM((row_count, 2 * hidden), jnp.bfloat16),
        ],
        input_output_aliases={7: 0, 8: 1},
        cost_estimate=pl.CostEstimate(
            flops=18 * count * row_count * width * hidden,
            bytes_accessed=4 * count * kinds * width * hidden + 16 * mix.size,
            transcendentals=count * row_count * hidden,
        ),
        name="expert_pass",
    )(*fixed, weights, mix, back)
    if packed:
        out = out.reshape(kinds, count, shards, depth, hidden).transpose(2, 0, 1, 3, 4)
    return (mix, back, out)


def swap(part):
    count = lax.axis_size("tensor")
    return lax.ppermute(part, "tensor", [(i, (i + 1) % count) for i in range(count)])


def both_halves(mine):
    other = swap(mine)
    first = lax.axis_index("tensor") == 0
    return jnp.concatenate(
        [jnp.where(first, mine, other), jnp.where(first, other, mine)], axis=0
    )


def sum_halves(part):
    half = part.shape[0] // 2
    place = lax.axis_index("tensor")
    mine = lax.dynamic_slice_in_dim(part, place * half, half, 0)
    given = lax.dynamic_slice_in_dim(part, (1 - place) * half, half, 0).astype(jnp.bfloat16)
    return mine.astype(jnp.bfloat16).astype(jnp.float32) + swap(given).astype(jnp.float32)


def scatter_sum(parts):
    place = lax.axis_index("dp")
    count = parts.shape[0]
    size = count
    bit = 1
    total = parts
    while size > 1:
        pairs = total.reshape((size // 2, 2) + parts.shape[1:])
        mine = (place // bit) % 2
        keep = lax.dynamic_index_in_dim(pairs, mine, 1, keepdims=False)
        give = lax.dynamic_index_in_dim(pairs, 1 - mine, 1, keepdims=False)
        taken = lax.ppermute(give, "dp", [(i, i ^ bit) for i in range(count)])
        total = keep.astype(jnp.float32) + taken.astype(jnp.float32)
        size //= 2
        bit *= 2
        if size > 1:
            total = total.astype(jnp.bfloat16)
    return total.reshape(parts.shape[1:])


def sum_everywhere(value):
    for axis in ("tensor", "dp"):
        count = lax.axis_size(axis)
        bit = 1
        while bit < count:
            value = value + lax.ppermute(value, axis, [(i, i ^ bit) for i in range(count)])
            bit *= 2
    return value


def local(
    tokens,
    out_grad,
    attn_norm,
    query_weight,
    key_weight,
    value_weight,
    output_weight,
    moe_norm,
    gate_weight,
    up_weight,
    down_weight,
    expert_ids,
    gate_weights,
    seq_lengths,
):
    expert_count = gate_weight.shape[0]
    heads_cols = query_weight.shape[1]
    kv_cols = key_weight.shape[1]
    qkv_cols = heads_cols + 2 * kv_cols
    dense_mine = jnp.concatenate([query_weight, key_weight, value_weight, output_weight], axis=1)
    dense_full = lax.all_gather(dense_mine, "dp", axis=0, tiled=True)
    qkv_full, output_full = dense_full[:, :qkv_cols], dense_full[:, qkv_cols:]
    stacked = (gate_weight, up_weight, down_weight)
    held = expert_count // GATHERS
    gathered = [
        lax.all_gather(jnp.stack([w[i * held : (i + 1) * held] for w in stacked]), "dp")
        for i in range(GATHERS)
    ]

    row_count = expert_ids.shape[0]
    doc_ids, positions, live_rows = row_layout(seq_lengths[0], row_count)
    cosine, sine_table = rope_tables(positions, HEAD_DIM)
    both = both_halves(jnp.concatenate([tokens, out_grad], axis=1))
    tokens_all, grad_all = both[:, : tokens.shape[1]], both[:, tokens.shape[1] :]
    widened = tokens.astype(jnp.float32)
    unit_attn, inv_attn = rms_rows(widened)
    unit_all, _ = rms_rows(tokens_all.astype(jnp.float32))
    normed_all = (unit_all * attn_norm).astype(jnp.bfloat16)
    head_count = heads_cols // HEAD_DIM
    kv_count = kv_cols // HEAD_DIM
    qkv = plain_dot(normed_all, qkv_full)
    turned = rotate(
        qkv[:, : heads_cols + kv_cols].reshape(row_count, head_count + kv_count, HEAD_DIM),
        cosine,
        sine_table,
    ).astype(jnp.bfloat16)
    queries, keys_rot = turned[:, :head_count], turned[:, head_count:]
    values = (
        qkv[:, heads_cols + kv_cols :]
        .astype(jnp.bfloat16)
        .reshape(row_count, kv_count, HEAD_DIM)
    )
    attn_rows, log_totals = attend(queries, keys_rot, values, doc_ids, live_rows)
    attn_flat = attn_rows.reshape(row_count, head_count * HEAD_DIM)
    after_attn = widened + sum_halves(times_t(attn_flat, output_full))
    unit_moe, inv_moe = rms_rows(after_attn)
    expert_in = (unit_moe * moe_norm).astype(jnp.bfloat16)
    expert_all = both_halves(expert_in)

    gates = expert_gates(expert_ids, gate_weights, live_rows, expert_count)
    fixed = (expert_all, expert_all.T, grad_all, grad_all.T, gates, gates.T)
    mix_part = jnp.zeros(expert_all.shape, jnp.float32)
    moe_part = jnp.zeros(expert_all.shape, jnp.float32)
    summed_experts = []
    count = expert_count // PASSES
    for low in range(0, expert_count, count):
        weights, offset = gathered[low // held], low % held
        mix_part, moe_part, grads = expert_pass(
            low, count, offset, *fixed, weights, mix_part, moe_part
        )
        summed_experts.append(scatter_sum(grads))

    moe_grad = sum_halves(moe_part)
    back_moe, grad_moe_norm = norm_back(moe_grad, unit_moe, inv_moe, moe_norm)
    resid_grad = out_grad.astype(jnp.float32) + back_moe
    resid_all = both_halves(resid_grad.astype(jnp.bfloat16))
    mixed = sum_halves(mix_part)
    block_out = (after_attn + mixed).astype(jnp.bfloat16)
    output_sum = scatter_sum(
        inner_rows(resid_all, attn_flat)
        .astype(jnp.bfloat16)
        .reshape(lax.axis_size("dp"), -1, heads_cols),
    )
    attn_grad = (
        plain_dot(resid_all, output_full)
        .astype(jnp.bfloat16)
        .reshape(row_count, head_count, HEAD_DIM)
    )
    query_grad, key_grad, value_grad = attend_back(
        queries, keys_rot, values, attn_rows, log_totals, attn_grad, doc_ids, live_rows
    )
    query_pre = (
        rotate_back(query_grad, cosine, sine_table).astype(jnp.bfloat16).reshape(row_count, -1)
    )
    key_pre = rotate_back(key_grad, cosine, sine_table).astype(jnp.bfloat16).reshape(row_count, -1)
    value_pre = value_grad.astype(jnp.bfloat16).reshape(row_count, -1)
    pre_all = jnp.concatenate([query_pre, key_pre, value_pre], axis=1)
    shards = lax.axis_size("dp")
    qkv_sum = scatter_sum(
        inner_rows(normed_all, pre_all).astype(jnp.bfloat16).reshape(shards, -1, qkv_cols),
    )
    attn_in_grad = sum_halves(times_t(pre_all, qkv_full))
    back_attn, grad_attn_norm = norm_back(attn_in_grad, unit_attn, inv_attn, attn_norm)
    input_grad = resid_grad + back_attn
    gain_sums = sum_everywhere(jnp.stack([grad_attn_norm, grad_moe_norm]))
    expert_sum = jnp.concatenate(summed_experts, axis=1)
    return (
        block_out,
        input_grad,
        gain_sums[0],
        qkv_sum[:, :heads_cols],
        qkv_sum[:, heads_cols : heads_cols + kv_cols],
        qkv_sum[:, heads_cols + kv_cols :],
        output_sum,
        gain_sums[1],
        expert_sum[0],
        expert_sum[1],
        expert_sum[2],
    )


def solution(mesh):
    in_specs = (
        P(("dp", "tensor"), None),
        P(("dp", "tensor"), None),
        P(),
        P("dp", "tensor"),
        P("dp", "tensor"),
        P("dp", "tensor"),
        P("dp", "tensor"),
        P(),
        P(None, "dp", "tensor"),
        P(None, "dp", "tensor"),
        P(None, "dp", "tensor"),
        P("dp", None),
        P("dp", None),
        P("dp", None),
    )
    out_specs = (
        P(("dp", "tensor"), None),
        P(("dp", "tensor"), None),
        P(),
        P("dp", "tensor"),
        P("dp", "tensor"),
        P("dp", "tensor"),
        P("dp", "tensor"),
        P(),
        P(None, "dp", "tensor"),
        P(None, "dp", "tensor"),
        P(None, "dp", "tensor"),
    )

    return jax.shard_map(local, mesh=mesh, in_specs=in_specs, out_specs=out_specs, check_vma=False)
```

```python
import functools
import math

import jax
import jax.numpy as jnp
from jax import lax
from jax.experimental import pallas as pl
from jax.experimental.pallas import tpu as pltpu
from jax.sharding import PartitionSpec as P

HEAD_DIM = 64
BLOCK = 128
PASSES = 5
FIRST_PASSES = 3


EPSILON = 1e-06
ROPE_BASE = 10000.0
MASKED = -1e30


def batched(pattern, first_op, second_op):
    return jnp.einsum(pattern, first_op, second_op, preferred_element_type=jnp.float32)


def times_t(first_op, weight):
    return lax.dot_general(
        first_op, weight, (((1,), (1,)), ((), ())), preferred_element_type=jnp.float32
    )


def plain_dot(first_op, weight):
    return jnp.dot(first_op, weight, preferred_element_type=jnp.float32)


def inner_rows(first_op, second_op):
    return lax.dot_general(
        first_op, second_op, (((0,), (0,)), ((), ())), preferred_element_type=jnp.float32
    )


def rms_rows(widened):
    inv_rms = lax.rsqrt(jnp.mean(widened * widened, axis=-1, keepdims=True) + EPSILON)
    return (widened * inv_rms, inv_rms)


def norm_back(grad_in, unit_rows, inv_rms, gain):
    scaled = grad_in * gain
    back = inv_rms * (scaled - unit_rows * jnp.mean(scaled * unit_rows, axis=-1, keepdims=True))
    return (back, jnp.sum(grad_in * unit_rows, axis=0))


def row_layout(lengths, row_count):
    padded = (lengths + BLOCK - 1) // BLOCK * BLOCK
    seq_ends = jnp.cumsum(padded)
    starts = seq_ends - padded
    row_ids = jnp.arange(row_count, dtype=jnp.int32)
    doc_ids = jnp.sum((row_ids[:, None] >= seq_ends[None, :]).astype(jnp.int32), axis=1)
    chosen = doc_ids[:, None] == jnp.arange(lengths.shape[0], dtype=jnp.int32)[None, :]
    first_row = jnp.sum(jnp.where(chosen, starts[None, :], 0), axis=1)
    length_row = jnp.sum(jnp.where(chosen, lengths[None, :], 0), axis=1)
    positions = row_ids - first_row
    return (doc_ids, positions, positions < length_row)


def rope_tables(positions, width):
    frequency = jnp.exp(
        jnp.arange(width // 2, dtype=jnp.int32).astype(jnp.float32)
        * (-2.0 * math.log(ROPE_BASE) / width)
    )
    angles = positions.astype(jnp.float32)[:, None] * frequency[None, :]
    cosine = jnp.cos(angles)
    sine_table = jnp.sin(angles)
    return (
        jnp.concatenate([cosine, cosine], axis=1),
        jnp.concatenate([sine_table, sine_table], axis=1),
    )


def rotate(values, cosine, sine_table):
    half_width = values.shape[-1] // 2
    turned = jnp.concatenate([-values[..., half_width:], values[..., :half_width]], axis=-1)
    return values * cosine[:, None, :] + turned * sine_table[:, None, :]


def rotate_back(grads, cosine, sine_table):
    half_width = grads.shape[-1] // 2
    turned = jnp.concatenate([grads[..., half_width:], -grads[..., :half_width]], axis=-1)
    return grads * cosine[:, None, :] + turned * sine_table[:, None, :]


def block_span(row_count):
    return min(512, row_count)


def allowed_block(first_row, block_rows, doc_ids, live_rows):
    row_count = doc_ids.shape[0]
    query_rows = first_row + jnp.arange(block_rows, dtype=jnp.int32)
    key_rows = jnp.arange(row_count, dtype=jnp.int32)
    same_doc = (key_rows[None, :] <= query_rows[:, None]) & (doc_ids[None, :] == doc_ids[:, None])
    same_doc = same_doc & live_rows[None, :] & live_rows[:, None]
    return same_doc | (key_rows[None, :] == query_rows[:, None])


def attend(queries, keys_rot, values, doc_ids, live_rows):
    row_count, head_count, head_width = queries.shape
    group_size = head_count // keys_rot.shape[1]
    keys_wide = jnp.repeat(keys_rot, group_size, axis=1)
    values_wide = jnp.repeat(values, group_size, axis=1)
    block_rows = block_span(row_count)
    block_count = row_count // block_rows
    score_scale = head_width ** (-0.5)

    def one_block(block_index):
        first_row = block_index * block_rows
        scores = batched("qhd,khd->hqk", queries, keys_wide) * score_scale
        scores = jnp.where(
            allowed_block(first_row, block_rows, doc_ids, live_rows)[None], scores, MASKED
        )
        highest = jnp.max(scores, axis=-1, keepdims=True)
        weights_exp = jnp.exp(scores - highest)
        totals = jnp.sum(weights_exp, axis=-1, keepdims=True)
        probability = (weights_exp / totals).astype(jnp.bfloat16)
        log_total = (highest + jnp.log(totals))[:, :, 0]
        return (batched("hqk,khd->qhd", probability, values_wide).astype(jnp.bfloat16), log_total)

    attn_blocks, log_totals = lax.map(one_block, jnp.arange(block_count, dtype=jnp.int32))
    return (attn_blocks.reshape(row_count, head_count, head_width), log_totals)


def attend_back(queries, keys_rot, values, attn_rows, log_totals, attn_grad, doc_ids, live_rows):
    row_count, head_count, head_width = queries.shape
    kv_count = keys_rot.shape[1]
    group_size = head_count // kv_count
    keys_wide = jnp.repeat(keys_rot, group_size, axis=1)
    values_wide = jnp.repeat(values, group_size, axis=1)
    block_rows = block_span(row_count)
    block_count = row_count // block_rows
    score_scale = head_width ** (-0.5)

    def one_block(running, block_index):
        key_acc, value_acc = running
        first_row = block_index * block_rows
        scores = batched("qhd,khd->hqk", queries, keys_wide) * score_scale
        scores = jnp.where(
            allowed_block(first_row, block_rows, doc_ids, live_rows)[None], scores, MASKED
        )
        probability = jnp.exp(scores - log_totals[block_index][:, :, None])
        value_acc = value_acc + batched("hqk,qhd->khd", probability.astype(jnp.bfloat16), attn_grad)
        through = batched("qhd,khd->hqk", attn_grad, values_wide)
        diagonal = jnp.sum(attn_grad.astype(jnp.float32) * attn_rows.astype(jnp.float32), axis=-1).T
        score_grad = (probability * (through - diagonal[:, :, None])).astype(jnp.bfloat16)
        query_grad = batched("hqk,khd->qhd", score_grad, keys_wide) * score_scale
        key_acc = key_acc + batched("hqk,qhd->khd", score_grad, queries) * score_scale
        return ((key_acc, value_acc), query_grad)

    zero_heads = jnp.zeros((row_count, head_count, head_width), jnp.float32)
    (key_acc, value_acc), query_grads = lax.scan(
        one_block, (zero_heads, zero_heads), jnp.arange(block_count, dtype=jnp.int32)
    )
    query_grad = query_grads.reshape(row_count, head_count, head_width)
    key_grad = key_acc.reshape(row_count, kv_count, group_size, head_width).sum(axis=2)
    value_grad = value_acc.reshape(row_count, kv_count, group_size, head_width).sum(axis=2)
    return (query_grad, key_grad, value_grad)


def silu_parts(gate_pre):
    sigma = jax.nn.sigmoid(gate_pre)
    return (gate_pre * sigma, sigma * (1.0 + gate_pre * (1.0 - sigma)))


def expert_gates(expert_ids, gate_weights, live_rows, expert_count):
    named = expert_ids[:, :, None] == jnp.arange(expert_count, dtype=jnp.int32)[None, None, :]
    named = named & live_rows[:, None, None]
    return jnp.sum(jnp.where(named, gate_weights[:, :, None], 0.0), axis=1)


def expert_kernel(
    first_expert,
    row_tile,
    feat_tile,
    mine_ref,
    rows_ref,
    rows_t_ref,
    grads_ref,
    grads_t_ref,
    gates_ref,
    gates_t_ref,
    weights_ref,
    *refs,
):
    if first_expert:
        mix_in_ref, back_in_ref, *refs = refs
    mix_ref, back_ref, keep_ref, give_ref, act_ref, pair_ref = refs
    step = pl.program_id(0)
    expert = first_expert + step
    row_count, width = rows_ref.shape
    _, hidden = weights_ref.shape[3:]

    @pl.when(step == 0)
    def _():
        if first_expert:
            mix_ref[...] = mix_in_ref[...]
            back_ref[...] = back_in_ref[...]
        else:
            mix_ref[...] = jnp.zeros_like(mix_ref)
            back_ref[...] = jnp.zeros_like(back_ref)

    gate_w = weights_ref[:, 0, 0].reshape(width, hidden)
    up_w = weights_ref[:, 1, 0].reshape(width, hidden)
    down_w = weights_ref[:, 2, 0].reshape(width, hidden)
    lanes = lax.broadcasted_iota(jnp.int32, (row_tile, gates_ref.shape[1]), 1)
    for start in range(0, row_count, row_tile):
        rows = slice(start, start + row_tile)
        gate_col = jnp.sum(
            jnp.where(lanes == expert, gates_ref[rows, :], 0.0), axis=1, keepdims=True
        )
        gate_pre = plain_dot(rows_ref[rows, :], gate_w)
        up_pre = plain_dot(rows_ref[rows, :], up_w)
        silu_val, slope = silu_parts(gate_pre)
        activ = (silu_val * up_pre).astype(jnp.bfloat16)
        act_ref[rows, :] = activ
        slot_grad = (grads_ref[rows, :].astype(jnp.float32) * gate_col).astype(jnp.bfloat16)
        act_grad = plain_dot(slot_grad, down_w)
        gate_grad = (act_grad * up_pre * slope).astype(jnp.bfloat16)
        up_grad = (act_grad * silu_val).astype(jnp.bfloat16)
        pair_ref[rows, :hidden] = gate_grad
        pair_ref[rows, hidden:] = up_grad
        mix_ref[rows, :] += times_t(activ, down_w) * gate_col
        back_ref[rows, :] += times_t(gate_grad, gate_w) + times_t(up_grad, up_w)
    gate_row = gates_t_ref[pl.ds(expert, 1), :]
    per_tile = feat_tile // keep_ref.shape[3]
    mine = mine_ref[0]
    for out_ref, parity in ((give_ref, 1 - mine), (keep_ref, mine)):
        for tile in range(rows_t_ref.shape[1] // feat_tile):
            feats = slice(tile * feat_tile, (tile + 1) * feat_tile)
            parts = slice(tile * per_tile, (tile + 1) * per_tile)
            shape = (per_tile,) + keep_ref.shape[3:]
            pair = plain_dot(rows_t_ref[parity, feats, :], pair_ref[...]).astype(jnp.bfloat16)
            out_ref[parts, 0, 0] = pair[:, :hidden].reshape(shape)
            out_ref[parts, 1, 0] = pair[:, hidden:].reshape(shape)
            slot_grad_t = (
                grads_t_ref[parity, feats, :].astype(jnp.float32) * gate_row
            ).astype(jnp.bfloat16)
            down = plain_dot(slot_grad_t, act_ref[...]).astype(jnp.bfloat16)
            out_ref[parts, 2, 0] = down.reshape(shape)


def by_parity(rows, shards):
    row_count, width = rows.shape
    split = rows.T.reshape(shards // 2, 2, width // shards, row_count)
    return split.transpose(1, 0, 2, 3).reshape(2, width // 2, row_count)


def expert_pass(first_expert, count, offset, mine, rows, rows_t, grads, grads_t, gates, gates_t, weights, mix, back):
    shards, kinds, held, depth, hidden = weights.shape
    row_count, width = rows.shape
    packed = depth % 16 != 0
    if packed:
        weights = weights.transpose(1, 2, 0, 3, 4).reshape(1, kinds, held, width, hidden)
    groups, inner = weights.shape[0], weights.shape[3]
    half_groups, half_inner = (1, width // 2) if packed else (shards // 2, depth)
    feat_tile = half_inner
    while feat_tile < 384 and (width // 2 // feat_tile) % 2 == 0:
        feat_tile *= 2

    def whole(array):
        return pl.BlockSpec(array.shape, lambda i: (0,) * array.ndim, pipeline_mode=pl.Buffered(1))

    shape = (groups, kinds, 1, inner, hidden)
    block = pl.BlockSpec(shape, lambda i: (0, 0, i + offset, 0, 0))
    half = pl.BlockSpec(
        (half_groups, kinds, 1, half_inner, hidden), lambda i: (0, 0, i, 0, 0)
    )
    fixed = (rows, rows_t, grads, grads_t, gates, gates_t)
    sums = (mix, back) if first_expert else ()
    mix, back, keep, give = pl.pallas_call(
        functools.partial(expert_kernel, first_expert, min(256, row_count), feat_tile),
        grid=(count,),
        in_specs=[pl.BlockSpec(memory_space=pltpu.SMEM)]
        + [whole(a) for a in fixed]
        + [block]
        + [whole(a) for a in sums],
        out_specs=[whole(rows), whole(rows), half, half],
        out_shape=[
            jax.ShapeDtypeStruct(rows.shape, jnp.float32),
            jax.ShapeDtypeStruct(rows.shape, jnp.float32),
            jax.ShapeDtypeStruct((half_groups, kinds, count, half_inner, hidden), jnp.bfloat16),
            jax.ShapeDtypeStruct((half_groups, kinds, count, half_inner, hidden), jnp.bfloat16),
        ],
        scratch_shapes=[
            pltpu.VMEM((row_count, hidden), jnp.bfloat16),
            pltpu.VMEM((row_count, 2 * hidden), jnp.bfloat16),
        ],
        input_output_aliases={8: 0, 9: 1} if first_expert else {},
        cost_estimate=pl.CostEstimate(
            flops=18 * count * row_count * width * hidden,
            bytes_accessed=4 * count * kinds * width * hidden + 16 * rows.size,
            transcendentals=count * row_count * hidden,
        ),
        name="expert_pass",
    )(mine, *fixed, weights, *sums)
    if packed:
        keep, give = (
            part.reshape(kinds, count, shards // 2, depth, hidden).transpose(2, 0, 1, 3, 4)
            for part in (keep, give)
        )
    return (mix, back, keep, give)


def swap(part):
    count = lax.axis_size("tensor")
    return lax.ppermute(part, "tensor", [(i, (i + 1) % count) for i in range(count)])


def both_halves(mine):
    other = swap(mine)
    first = lax.axis_index("tensor") == 0
    return jnp.concatenate(
        [jnp.where(first, mine, other), jnp.where(first, other, mine)], axis=0
    )


def both_columns(mine):
    other = swap(mine)
    first = lax.axis_index("tensor") == 0
    return jnp.concatenate(
        [jnp.where(first, mine, other), jnp.where(first, other, mine)], axis=-1
    )


def half_of(whole):
    half = whole.shape[0] // 2
    return lax.dynamic_slice_in_dim(whole, lax.axis_index("tensor") * half, half, 0)


def sum_halves(part):
    half = part.shape[0] // 2
    place = lax.axis_index("tensor")
    mine = lax.dynamic_slice_in_dim(part, place * half, half, 0)
    given = lax.dynamic_slice_in_dim(part, (1 - place) * half, half, 0).astype(jnp.bfloat16)
    return mine.astype(jnp.bfloat16).astype(jnp.float32) + swap(given).astype(jnp.float32)


def scatter_sum(keep, give, swapped=False):
    place = lax.axis_index("dp")
    count = lax.axis_size("dp")
    left = [1 << i for i in range(count.bit_length() - 1)]
    bit = left.pop(0)
    while True:
        taken = lax.ppermute(give, "dp", [(i, i ^ bit) for i in range(count)])
        if not left:
            return (keep.astype(jnp.float32) + taken.astype(jnp.float32))[0]
        low = 1 if swapped and len(left) > 1 else 0
        swapped = False
        bit = left.pop(low)
        tail = keep.shape[1:]
        shape = (keep.shape[0] >> (low + 1), 2, 1 << low) + tail
        mine = (place // bit) % 2

        def added(which):
            first = lax.dynamic_index_in_dim(keep.reshape(shape), which, 1, keepdims=False)
            second = lax.dynamic_index_in_dim(taken.reshape(shape), which, 1, keepdims=False)
            total = first.astype(jnp.float32) + second.astype(jnp.float32)
            return total.astype(jnp.bfloat16).reshape((-1,) + tail)

        give, keep = added(1 - mine), added(mine)


def sum_everywhere(value):
    for axis in ("tensor", "dp"):
        count = lax.axis_size(axis)
        bit = 1
        while bit < count:
            other = lax.ppermute(value, axis, [(i, i ^ bit) for i in range(count)])
            value = value + other
            bit *= 2
    return value


def scatter_rows(product):
    count = lax.axis_size("dp")
    mine = lax.axis_index("dp") % 2
    pairs = product.reshape((count // 2, 2, product.shape[0] // count) + product.shape[1:])
    give = lax.dynamic_index_in_dim(pairs, 1 - mine, 1, keepdims=False)
    keep = lax.dynamic_index_in_dim(pairs, mine, 1, keepdims=False)
    return scatter_sum(keep, give)


def gather_rows(block, across=False):
    place = lax.axis_index("dp")
    count = lax.axis_size("dp")
    held = block[None]
    bit = count // 2
    while bit:
        if across and bit == 2:
            held = both_columns(held)
        other = lax.ppermute(held, "dp", [(i, i ^ bit) for i in range(count)])
        first = (place // bit) % 2 == 0
        tail = held.shape[1:]
        held = jnp.stack([jnp.where(first, held, other), jnp.where(first, other, held)], axis=1)
        held = held.reshape((-1,) + tail)
        bit //= 2
    return held.reshape((-1,) + held.shape[2:])


def local(
    tokens,
    out_grad,
    attn_norm,
    query_weight,
    key_weight,
    value_weight,
    output_weight,
    moe_norm,
    gate_weight,
    up_weight,
    down_weight,
    expert_ids,
    gate_weights,
    seq_lengths,
):
    expert_count = gate_weight.shape[0]
    heads_cols = query_weight.shape[1]
    kv_cols = key_weight.shape[1]
    qkv_full = gather_rows(jnp.concatenate([query_weight, key_weight, value_weight], axis=1))
    output_all = gather_rows(output_weight, across=True)
    stacked = (gate_weight, up_weight, down_weight)
    count = expert_count // PASSES
    split = FIRST_PASSES * count
    gathered = [
        lax.all_gather(jnp.stack([w[low:high] for w in stacked]), "dp")
        for low, high in ((0, split), (split, expert_count))
    ]

    row_count = expert_ids.shape[0]
    doc_ids, positions, live_rows = row_layout(seq_lengths[0], row_count)
    cosine, sine_table = rope_tables(positions, HEAD_DIM)
    both = both_halves(jnp.concatenate([tokens, out_grad], axis=1))
    tokens_all, grad_all = both[:, : tokens.shape[1]], both[:, tokens.shape[1] :]
    widened = tokens.astype(jnp.float32)
    unit_attn, inv_attn = rms_rows(widened)
    unit_all, _ = rms_rows(tokens_all.astype(jnp.float32))
    normed_all = (unit_all * attn_norm).astype(jnp.bfloat16)
    head_count = heads_cols // HEAD_DIM
    kv_count = kv_cols // HEAD_DIM
    qkv = plain_dot(normed_all, qkv_full)
    turned = rotate(
        qkv[:, : heads_cols + kv_cols].reshape(row_count, head_count + kv_count, HEAD_DIM),
        cosine,
        sine_table,
    ).astype(jnp.bfloat16)
    queries, keys_rot = turned[:, :head_count], turned[:, head_count:]
    values = (
        qkv[:, heads_cols + kv_cols :]
        .astype(jnp.bfloat16)
        .reshape(row_count, kv_count, HEAD_DIM)
    )
    attn_rows, log_totals = attend(queries, keys_rot, values, doc_ids, live_rows)
    attn_flat = attn_rows.reshape(row_count, head_count * HEAD_DIM)
    attn_all = both_columns(attn_flat)
    after_all = tokens_all.astype(jnp.float32) + times_t(attn_all, output_all)
    moe_all, moe_inv_all = rms_rows(after_all)
    expert_all = (moe_all * moe_norm).astype(jnp.bfloat16)
    after_attn = half_of(after_all)
    unit_moe, inv_moe = half_of(moe_all), half_of(moe_inv_all)

    gates = expert_gates(expert_ids, gate_weights, live_rows, expert_count)
    shards = lax.axis_size("dp")
    fixed = (
        expert_all,
        by_parity(expert_all, shards),
        grad_all,
        by_parity(grad_all, shards),
        gates,
        gates.T,
    )
    parity = (lax.axis_index("dp") % 2).astype(jnp.int32).reshape(1)
    mix_part = moe_part = None
    summed_experts = []
    for low in range(0, expert_count, count):
        weights, offset = gathered[low >= split], low % split
        mix_part, moe_part, keep, give = expert_pass(
            low, count, offset, parity, *fixed, weights, mix_part, moe_part
        )
        summed_experts.append(scatter_sum(keep, give, low == 0))

    moe_grad = sum_halves(moe_part)
    back_moe, grad_moe_norm = norm_back(moe_grad, unit_moe, inv_moe, moe_norm)
    resid_grad = out_grad.astype(jnp.float32) + back_moe
    resid_half = resid_grad.astype(jnp.bfloat16)
    by_heads = plain_dot(resid_half, output_all).astype(jnp.bfloat16)
    place = lax.axis_index("tensor")
    own_heads = lax.dynamic_slice_in_dim(by_heads, place * heads_cols, heads_cols, 1)
    their_rows = swap(lax.dynamic_slice_in_dim(by_heads, (1 - place) * heads_cols, heads_cols, 1))
    attn_grad = jnp.concatenate(
        [
            jnp.where(place == 0, own_heads, their_rows),
            jnp.where(place == 0, their_rows, own_heads),
        ],
        axis=0,
    ).reshape(row_count, head_count, HEAD_DIM)
    resid_all = both_halves(resid_half)
    mixed = sum_halves(mix_part)
    block_out = (after_attn + mixed).astype(jnp.bfloat16)
    output_sum = scatter_rows(inner_rows(resid_all, attn_flat).astype(jnp.bfloat16))
    query_grad, key_grad, value_grad = attend_back(
        queries, keys_rot, values, attn_rows, log_totals, attn_grad, doc_ids, live_rows
    )
    query_pre = (
        rotate_back(query_grad, cosine, sine_table).astype(jnp.bfloat16).reshape(row_count, -1)
    )
    key_pre = rotate_back(key_grad, cosine, sine_table).astype(jnp.bfloat16).reshape(row_count, -1)
    value_pre = value_grad.astype(jnp.bfloat16).reshape(row_count, -1)
    pre_all = jnp.concatenate([query_pre, key_pre, value_pre], axis=1)
    qkv_sum = scatter_rows(inner_rows(normed_all, pre_all).astype(jnp.bfloat16))
    attn_in_grad = sum_halves(times_t(pre_all, qkv_full))
    back_attn, grad_attn_norm = norm_back(attn_in_grad, unit_attn, inv_attn, attn_norm)
    input_grad = resid_grad + back_attn
    gain_sums = sum_everywhere(jnp.stack([grad_attn_norm, grad_moe_norm]))
    expert_sum = jnp.concatenate(summed_experts, axis=1)
    return (
        block_out,
        input_grad,
        gain_sums[0],
        qkv_sum[:, :heads_cols],
        qkv_sum[:, heads_cols : heads_cols + kv_cols],
        qkv_sum[:, heads_cols + kv_cols :],
        output_sum,
        gain_sums[1],
        expert_sum[0],
        expert_sum[1],
        expert_sum[2],
    )


def solution(mesh):
    in_specs = (
        P(("dp", "tensor"), None),
        P(("dp", "tensor"), None),
        P(),
        P("dp", "tensor"),
        P("dp", "tensor"),
        P("dp", "tensor"),
        P("dp", "tensor"),
        P(),
        P(None, "dp", "tensor"),
        P(None, "dp", "tensor"),
        P(None, "dp", "tensor"),
        P("dp", None),
        P("dp", None),
        P("dp", None),
    )
    out_specs = (
        P(("dp", "tensor"), None),
        P(("dp", "tensor"), None),
        P(),
        P("dp", "tensor"),
        P("dp", "tensor"),
        P("dp", "tensor"),
        P("dp", "tensor"),
        P(),
        P(None, "dp", "tensor"),
        P(None, "dp", "tensor"),
        P(None, "dp", "tensor"),
    )

    return jax.shard_map(local, mesh=mesh, in_specs=in_specs, out_specs=out_specs, check_vma=False)
```
